32 devices in a mesh: dp: 8 (over z, x), mp: 4 (over y, core).
Axes of the slice: x: 2, y: 2, z: 4, core: 2. Of those that a mesh axis runs over, the one named last changes fastest.
Arguments:
- vision_rows: bfloat16 [1024, 1024], P('dp'), may hold values from -6 to 6
- image_count: int32 [32], P('dp'), may hold values from 0 to 4
- proj_flat: bfloat16 [32768, 128], P(('dp', 'mp')), may hold values from -0.1875 to 0.1875
- text_embeds: bfloat16 [3072, 4096], P(('dp', 'mp')), may hold values from -6 to 6
- norm_gain: float32 [4096], replicated, may hold values from 0.1 to 1.9
- q_weight: bfloat16 [4096, 4096], P(None, 'mp'), may hold values from -0.09375 to 0.09375
- q_grad: bfloat16 [4096, 4096], P('dp', 'mp'), may hold values from -6 to 6
Outputs:
- text_grad: bfloat16 [3072, 4096], P(('dp', 'mp'))
- proj_grad: float32 [32768, 128], P(('dp', 'mp'))
The draws below stay inside these ranges and needn't reach their ends.
Inputs may be any that keep to these rules, and one draw needn't show every extreme that they name: Slot s of device k holds an image when s < image_count[k]; other slots are padding.
All inputs are finite; a program needn't handle non-finite values.
Results may differ from the reference program's by a relative error of at most 0.014.
Values may be sent and summed in bfloat16 or wider, within the bound.
A program may use at most 64 MiB of HBM per device.

```python
import jax
import jax.numpy as jnp
from jax import lax

D = 4096
ENC = 1024
IMG_MAX = 4
PATCH = 8
TEXT_DEV = 96
IMG_ROWS = 32
ROWS_DEV = 128
PROJ_ROWS = 1024
N_DP = 8
N_MP = 4


def plant(drawn, own_key, least, largest):
    longest = drawn.shape.index(max(drawn.shape))
    spots = []
    for shift in (0, 1):
        where = [jax.random.randint(jax.random.fold_in(own_key, axis), (), 0, length) for axis, length in enumerate(drawn.shape)]
        where[longest] = (where[longest] + shift) % drawn.shape[longest]
        spots.append(tuple(where))
    return drawn.at[spots[0]].set(least).at[spots[1]].set(largest)


def block_scale(key, extent, cuts, smallest, high):
    level = 1.0
    for position, blocks in cuts:
        heights = jax.random.uniform(jax.random.fold_in(jax.random.fold_in(key, 6), position), (blocks,), jnp.float32, smallest / len(cuts), high / len(cuts))
        level = level * jnp.repeat(jnp.exp(heights), extent[position] // blocks).reshape((-1,) + (1,) * (len(extent) - 1 - position))
    return level


def bell_draw(own_key, dims, deviation, most, split=(), kind=jnp.bfloat16):
    gain = block_scale(own_key, dims, split, -0.22, 0.18) if split else 1.0
    array = jax.random.normal(own_key, dims, jnp.float32) * deviation * gain
    return jnp.minimum(jnp.maximum(array, -most), most).astype(kind)


def setup_inputs(seed: int = 0) -> dict:
    streams_of = jax.random.split(jax.random.key(seed), 8)
    vision_rows = bell_draw(streams_of[0], (N_DP * N_MP * IMG_ROWS, ENC), 1.0, 6.0, ((0, 8),))
    image_count = plant(jax.random.randint(streams_of[1], (N_DP * N_MP,), 0, IMG_MAX + 1), jax.random.fold_in(streams_of[1], 1), 0, IMG_MAX).astype(jnp.int32)
    proj_flat = bell_draw(streams_of[2], (N_DP * N_MP * PROJ_ROWS, 128), ENC ** -0.5, 0.1875, ((0, 32),))
    text_embeds = bell_draw(streams_of[3], (N_DP * N_MP * TEXT_DEV, D), 1.0, 6.0, ((0, 32),))
    norm_gain = jnp.clip(1.0 + 0.18 * jax.random.normal(streams_of[4], (D,), jnp.float32), 0.1, 1.9)
    q_weight = bell_draw(streams_of[5], (D, D), D ** -0.5, 0.09375, ((1, 4),))
    q_grad = bell_draw(streams_of[6], (N_DP * N_MP * ROWS_DEV, D), 1.0, 6.0, ((0, 8), (1, 4)))
    return {"vision_rows": vision_rows, "image_count": image_count, "proj_flat": proj_flat, "text_embeds": text_embeds, "norm_gain": norm_gain, "q_weight": q_weight, "q_grad": q_grad}


norm_eps = 1e-05

def reference(vision_rows, image_count, proj_flat, text_embeds, norm_gain, q_weight, q_grad):
    block_cols = D // N_MP
    used_count = ENC * block_cols
    stored = proj_flat.reshape(N_DP, N_MP, PROJ_ROWS * 128).transpose(1, 0, 2)
    stored = stored.reshape(N_MP, N_DP * PROJ_ROWS * 128)[:, :used_count]
    proj_weight = stored.reshape(N_MP, ENC, block_cols).transpose(1, 0, 2).reshape(ENC, D)
    image_embed = jnp.dot(vision_rows, proj_weight, preferred_element_type=jnp.float32).astype(jnp.bfloat16)
    image_blocks = image_embed.reshape(N_DP * N_MP, IMG_ROWS, D)
    text_blocks = text_embeds.reshape(N_DP * N_MP, TEXT_DEV, D)
    decoder_in = jnp.concatenate([image_blocks, text_blocks], axis=1).reshape(-1, D)
    inputs = decoder_in.astype(jnp.float32)
    inv_rms = lax.rsqrt(lax.optimization_barrier(jnp.mean(inputs * inputs, axis=-1, keepdims=True)) + norm_eps)
    norm_grad = jnp.zeros(inputs.shape, jnp.float32)
    for member in range(N_MP):
        left = q_grad[:, member * block_cols:(member + 1) * block_cols]
        right = q_weight[:, member * block_cols:(member + 1) * block_cols]
        term = jnp.dot(left, right.T, preferred_element_type=jnp.float32).astype(jnp.bfloat16)
        term = lax.optimization_barrier(term)
        norm_grad = norm_grad + term.astype(jnp.float32)
    scaled = norm_gain[None, :] * norm_grad
    inner_mean = lax.optimization_barrier(jnp.mean(scaled * inputs, axis=-1, keepdims=True))
    input_grad = inv_rms * scaled - inputs * inv_rms ** 3 * inner_mean
    grad_blocks = input_grad.reshape(N_DP * N_MP, ROWS_DEV, D)
    text_grad = grad_blocks[:, IMG_ROWS:, :].reshape(-1, D).astype(jnp.bfloat16)
    live_slots = jnp.arange(IMG_MAX, dtype=jnp.int32)[None, :] < image_count[:, None]
    live_rows = jnp.repeat(live_slots, PATCH, axis=1)
    image_grad = jnp.where(live_rows[:, :, None], grad_blocks[:, :IMG_ROWS, :], 0.0)
    image_grad = image_grad.reshape(-1, D).astype(jnp.bfloat16)
    grad_scale = 1.0 / jnp.sqrt(jnp.float32(N_DP * N_MP * IMG_ROWS))
    proj_full = jnp.dot(vision_rows.T, image_grad, preferred_element_type=jnp.float32) * grad_scale
    flat_blocks = proj_full.reshape(ENC, N_MP, block_cols).transpose(1, 0, 2).reshape(N_MP, used_count)
    flat_blocks = jnp.pad(flat_blocks, ((0, 0), (0, N_DP * PROJ_ROWS * 128 - used_count)))
    proj_grad = flat_blocks.reshape(N_MP, N_DP, PROJ_ROWS * 128).transpose(1, 0, 2)
    proj_grad = proj_grad.reshape(N_DP * N_MP * PROJ_ROWS, 128)
    return (text_grad, proj_grad)
```

```python
import functools

import jax
import jax.numpy as jnp
from jax import lax
from jax.experimental import pallas as pl
from jax.experimental.pallas import tpu as pltpu
from jax.sharding import PartitionSpec as P

IMG_MAX = 4
PATCH = 8
ROWS_DEV = 128
CORES = 2
SIDE = 2
CHUNKS = 2
TILE = 256
ROW_STEP = 16

MESH = pl.DeviceIdType.MESH

norm_eps = 1e-05


def row_term(left, weight):
    return lax.dot_general(
        left, weight, (((1,), (1,)), ((), ())), preferred_element_type=jnp.float32
    )


class LineGather:
    def __init__(self, depth, me, member, own, buf, send, recv):
        self.depth, self.me, self.member = depth, me, member
        self.z, self.x = me // SIDE, me % SIDE
        self.own, self.buf, self.send, self.recv = own, buf, send, recv
        self.step = buf.shape[1] // CHUNKS

    def rows(self, chunk):
        return pl.ds(chunk * self.step, self.step)

    def copy(self, zz, x, chunk, way, own=False):
        block = zz * SIDE + x
        place = self.buf.at[block, self.rows(chunk)]
        target = (self.me + SIDE, self.me - SIDE, self.z * SIDE + (1 - self.x))[way]
        return pltpu.make_async_remote_copy(
            src_ref=self.own.at[self.rows(chunk)] if own else place,
            dst_ref=place,
            send_sem=self.send.at[way, zz, chunk],
            recv_sem=self.recv.at[block, chunk],
            device_id=(target, self.member),
            device_id_type=MESH,
        )

    def start(self):
        for chunk in range(CHUNKS):
            @pl.when(self.z < self.depth - 1)
            def _():
                self.copy(self.z, self.x, chunk, 0, True).start()

            @pl.when(self.z > 0)
            def _():
                self.copy(self.z, self.x, chunk, 1, True).start()

            self.copy(self.z, self.x, chunk, 2, True).start()

    def relay(self, hop, chunk):
        below, above = self.z - hop, self.z + hop

        @pl.when(below >= 0)
        def _():
            self.copy(below, self.x, chunk, 0).wait_recv()

            @pl.when(self.z < self.depth - 1)
            def _():
                self.copy(below, self.x, chunk, 0).start()

            self.copy(below, self.x, chunk, 2).start()

        @pl.when(above < self.depth)
        def _():
            self.copy(above, self.x, chunk, 1).wait_recv()

            @pl.when(self.z > 0)
            def _():
                self.copy(above, self.x, chunk, 1).start()

            self.copy(above, self.x, chunk, 2).start()

    def line_blocks(self, hop, use):
        for zz in (self.z - hop, self.z + hop):
            @pl.when((zz >= 0) & (zz < self.depth))
            def _():
                use(zz * SIDE + self.x)

    def side_blocks(self, hop, use):
        for zz in (self.z,) if hop == 0 else (self.z - hop, self.z + hop):
            @pl.when((zz >= 0) & (zz < self.depth))
            def _():
                for chunk in range(CHUNKS):
                    self.copy(zz, 1 - self.x, chunk, 2).wait_recv()
                use(zz * SIDE + 1 - self.x)

    def drain(self):
        for zz in range(self.depth):
            for chunk in range(CHUNKS):
                @pl.when((self.z >= zz) & (self.z < self.depth - 1))
                def _():
                    self.copy(zz, self.x, chunk, 0).wait_send()

                @pl.when((self.z <= zz) & (self.z > 0))
                def _():
                    self.copy(zz, self.x, chunk, 1).wait_send()

                self.copy(zz, self.x, chunk, 2).wait_send()


def kernel(
    shards, groups, grad_scale,
    proj_ref, vision_ref, live_ref, gain_ref, q_hbm, w_hbm, text_hbm,
    text_out, proj_out,
    qv, wv, tv, own_text, own_image, mate_text, mate_image, sum_text, sum_image,
    far_text, far_image, scaled_image, x_acc, g_acc, g_own, stat_own, stats,
    w_all, g_all, v_all,
    q_sem, w_sem, t_sem, a_send, a_recv, c_send, c_recv, v_send, v_recv,
    mt_send, mt_recv, mi_send, mi_recv, ft_send, ft_recv, fi_send, fi_recv, s_send, s_recv,
):
    me, member = lax.axis_index("dp"), lax.axis_index("mp")
    depth = shards // SIDE
    chips = groups // CORES
    y, core = member // CORES, member % CORES
    mate = y * CORES + 1 - core
    shard_k, block_cols = proj_ref.shape
    image_rows = vision_ref.shape[0]
    per_image = image_rows // groups
    rows_dev = qv.shape[0] // groups
    text_rows = rows_dev - per_image
    width = groups * block_cols
    f32, bf16 = jnp.float32, jnp.bfloat16

    far = [lax.rem(y + step, chips) for step in range(1, chips)]
    order = [yy * CORES + lax.rem(core + flip, CORES) for yy in far + [y] for flip in (1, 0)]
    early = len(order) // 2

    q_copy = pltpu.make_async_copy(q_hbm, qv, q_sem)
    q_copy.start()
    w_copies = [pltpu.make_async_copy(w_hbm.at[j], wv.at[j], w_sem.at[k]) for k, j in enumerate(order)]
    for copy in w_copies:
        copy.start()
    t_copy = pltpu.make_async_copy(text_hbm, tv, t_sem)
    t_copy.start()

    barrier = pltpu.get_barrier_semaphore()
    for step in range(1, shards):
        pl.semaphore_signal(
            barrier, inc=1, device_id=(lax.rem(me + step, shards), member), device_id_type=MESH
        )
    for step in range(1, groups):
        pl.semaphore_signal(
            barrier, inc=1, device_id=(me, lax.rem(member + step, groups)), device_id_type=MESH
        )
    pl.semaphore_wait(barrier, shards + groups - 2)

    weights = LineGather(depth, me, member, proj_ref, w_all, a_send, a_recv)
    weights.start()

    def remote(src, dst, send, recv, device):
        return pltpu.make_async_remote_copy(
            src_ref=src, dst_ref=dst, send_sem=send, recv_sem=recv,
            device_id=device, device_id_type=MESH,
        )

    def text_to_mate(k):
        j = order[k]
        return remote(own_text.at[j, 1 - core], mate_text.at[j], mt_send.at[j], mt_recv.at[j], (me, mate))

    def image_to_mate(yy):
        return remote(
            own_image.at[yy * CORES + 1 - core], mate_image.at[yy],
            mi_send.at[yy], mi_recv.at[yy], (me, mate),
        )

    def text_to_far(k, yy):
        j = order[k]
        return remote(
            sum_text.at[j, yy], far_text.at[y, j], ft_send.at[j, yy], ft_recv.at[y, j],
            (me, yy * CORES + core),
        )

    def text_from_far(k, yy):
        j = order[k]
        return remote(
            sum_text.at[j, yy], far_text.at[yy, j], ft_send.at[j, yy], ft_recv.at[yy, j],
            (me, yy * CORES + core),
        )

    def image_to_far(yy):
        return remote(
            sum_image.at[yy], far_image.at[y], fi_send.at[yy], fi_recv.at[y], (me, yy * CORES + core)
        )

    def image_from_far(yy):
        return remote(
            sum_image.at[yy], far_image.at[yy], fi_send.at[yy], fi_recv.at[yy], (me, yy * CORES + core)
        )

    def multiply(k):
        j = order[k]
        w_copies[k].wait()

        @pl.loop(0, block_cols // TILE)
        def _(n):
            cols = pl.ds(pl.multiple_of(n * TILE, TILE), TILE)
            term = row_term(qv[...], wv[j, cols, :]).astype(bf16)
            for g in range(groups):
                base = g * rows_dev
                own_image[j, pl.ds(g * per_image, per_image), cols] = term[base : base + per_image]
                own_text[j, g % CORES, g // CORES, :, cols] = term[base + per_image : base + rows_dev]

        text_to_mate(k).start()

    def add_image(yy):
        image_to_mate(yy).wait_recv()

        @pl.loop(0, image_rows // ROW_STEP)
        def _(n):
            rows = pl.ds(pl.multiple_of(n * ROW_STEP, ROW_STEP), ROW_STEP)
            total = own_image[yy * CORES + core, rows].astype(f32) + mate_image[yy, rows].astype(f32)
            sum_image[yy, rows] = total.astype(bf16)

    def add_text(k):
        j = order[k]
        text_to_mate(k).wait_recv()
        for yy in far:
            @pl.loop(0, text_rows // ROW_STEP)
            def _(n):
                rows = pl.ds(pl.multiple_of(n * ROW_STEP, ROW_STEP), ROW_STEP)
                total = own_text[j, core, yy, rows].astype(f32) + mate_text[j, yy, rows].astype(f32)
                sum_text[j, yy, rows] = total.astype(bf16)

    def send_text(k):
        for yy in far:
            text_to_far(k, yy).start()

    q_copy.wait()
    for k in range(early):
        multiply(k)
        if k % CORES == 0:
            image_to_mate(far[k // CORES]).start() if k // CORES < len(far) else None
    for yy in far[: early // CORES]:
        add_image(yy)
        image_to_far(yy).start()
    weights.relay(1, 0)
    for k in range(early):
        add_text(k)
        send_text(k)
    for chunk in range(1, CHUNKS):
        weights.relay(1, chunk)
    for k in range(early, len(order)):
        multiply(k)
        if k % CORES == 0:
            image_to_mate((far + [y])[k // CORES]).start()
        if 2 < depth and k - early < CHUNKS:
            weights.relay(2, k - early)
    for yy in far[early // CORES :]:
        add_image(yy)
        image_to_far(yy).start()
    for chunk in range(len(order) - early, CHUNKS):
        weights.relay(2, chunk)

    def use_weights(block):
        cols = pl.ds(pl.multiple_of(block * shard_k, shard_k), shard_k)
        x_acc[...] += jnp.dot(vision_ref[:, cols], w_all[block], preferred_element_type=f32)

    own_cols = pl.ds(pl.multiple_of(me * shard_k, shard_k), shard_k)
    x_acc[...] = jnp.dot(vision_ref[:, own_cols], proj_ref[...], preferred_element_type=f32)
    weights.line_blocks(1, use_weights)
    for hop in range(3, depth):
        for chunk in range(CHUNKS):
            weights.relay(hop, chunk)
    for hop in range(2, depth):
        weights.line_blocks(hop, use_weights)

    def vision_to(step):
        target = lax.rem(me + step, shards)
        cols = pl.ds(pl.multiple_of(target * shard_k, shard_k), shard_k)
        return remote(
            vision_ref.at[:, cols], v_all.at[me], v_send.at[target], v_recv.at[me], (target, member)
        )

    def vision_from(step):
        source = lax.rem(me + step, shards)
        cols = pl.ds(pl.multiple_of(source * shard_k, shard_k), shard_k)
        return remote(
            vision_ref.at[:, cols], v_all.at[source], v_send.at[source], v_recv.at[source], (source, member)
        )

    for step in range(1, shards):
        vision_to(step).start()

    image_to_mate(y).wait_recv()
    for yy in far:
        image_from_far(yy).wait_recv()
    member_cols = pl.ds(pl.multiple_of(member * block_cols, block_cols), block_cols)

    @pl.loop(0, image_rows // ROW_STEP)
    def _(n):
        rows = pl.ds(pl.multiple_of(n * ROW_STEP, ROW_STEP), ROW_STEP)
        total = own_image[member, rows].astype(f32) + mate_image[y, rows].astype(f32)
        for yy in far:
            total = total + far_image[yy, rows].astype(f32)
        scaled_image[rows] = gain_ref[:, member_cols] * total

    for k in range(early, len(order)):
        add_text(k)
    for hop in range(depth):
        weights.side_blocks(hop, use_weights)

    @pl.loop(0, image_rows // ROW_STEP)
    def _(n):
        rows = pl.ds(pl.multiple_of(n * ROW_STEP, ROW_STEP), ROW_STEP)
        x = x_acc[rows].astype(bf16).astype(f32)
        x_acc[rows] = x
        squares = jnp.sum(x * x, axis=1, keepdims=True)
        inner = jnp.sum(x * scaled_image[rows], axis=1, keepdims=True)
        lane = lax.broadcasted_iota(jnp.int32, (ROW_STEP, 128), 1)
        g_acc[rows, pl.ds(0, 128)] = jnp.where(lane == 0, squares, inner)

    stat_own[...] = g_acc[:, 0:128].T[0:8]

    def stat_to(step):
        target = lax.rem(member + step, groups)
        return remote(stat_own, stats.at[member], s_send.at[target], s_recv.at[member], (me, target))

    def stat_from(step):
        source = lax.rem(member + step, groups)
        return remote(stat_own, stats.at[source], s_send.at[source], s_recv.at[source], (me, source))

    for step in range(1, groups):
        stat_to(step).start()
    for k in range(early, len(order)):
        send_text(k)
    total = stat_own[...]
    for step in range(1, groups):
        stat_from(step).wait_recv()
        total = total + stats[lax.rem(member + step, groups)]
    spread = jnp.concatenate([total] * 16, axis=0).T
    inv_all = lax.rsqrt(spread[:, 0:1] / width + norm_eps)
    g_acc[:, 0:128] = jnp.broadcast_to(inv_all, (image_rows, 128))
    g_acc[:, 128:256] = jnp.broadcast_to(inv_all**3 * (spread[:, 1:2] / width), (image_rows, 128))

    @pl.loop(0, image_rows // ROW_STEP)
    def _(n):
        rows = pl.ds(pl.multiple_of(n * ROW_STEP, ROW_STEP), ROW_STEP)
        inv, pull = g_acc[rows, pl.ds(0, 1)], g_acc[rows, pl.ds(128, 1)]
        grad = inv * scaled_image[rows] - x_acc[rows] * pull
        g_own[rows] = jnp.where(live_ref[rows] > 0, grad, 0.0).astype(bf16)

    grads = LineGather(depth, me, member, g_own, g_all, c_send, c_recv)
    grads.start()

    def vision_term(left, right):
        return lax.dot_general(left, right, (((0,), (0,)), ((), ())), preferred_element_type=f32)

    def use_grads(block):
        g_acc[...] += vision_term(v_all[block], g_all[block])

    g_acc[...] = vision_term(vision_ref[:, own_cols], g_own[...])
    for step in range(1, shards):
        vision_from(step).wait_recv()
    for hop in range(1, depth):
        for chunk in range(CHUNKS):
            grads.relay(hop, chunk)
        if hop < depth - 1:
            grads.line_blocks(hop, use_grads)
    grads.line_blocks(depth - 1, use_grads)

    for k in range(len(order)):
        for yy in far:
            text_from_far(k, yy).wait_recv()
    t_copy.wait()

    @pl.loop(0, text_rows // ROW_STEP)
    def _(n):
        rows = pl.ds(pl.multiple_of(n * ROW_STEP, ROW_STEP), ROW_STEP)
        squares = jnp.zeros((ROW_STEP, 1), f32)
        inner = jnp.zeros((ROW_STEP, 1), f32)
        for j in range(groups):
            cols = pl.ds(j * block_cols, block_cols)
            x = tv[rows, cols].astype(f32)
            norm = own_text[j, core, y, rows].astype(f32) + mate_text[j, y, rows].astype(f32)
            for yy in far:
                norm = norm + far_text[yy, j, rows].astype(f32)
            scaled = gain_ref[:, cols] * norm
            squares += jnp.sum(x * x, axis=1, keepdims=True)
            inner += jnp.sum(x * scaled, axis=1, keepdims=True)
        inv = lax.rsqrt(squares / width + norm_eps)
        pull = inv**3 * (inner / width)
        for j in range(groups):
            cols = pl.ds(j * block_cols, block_cols)
            x = tv[rows, cols].astype(f32)
            norm = own_text[j, core, y, rows].astype(f32) + mate_text[j, y, rows].astype(f32)
            for yy in far:
                norm = norm + far_text[yy, j, rows].astype(f32)
            text_out[rows, cols] = (inv * (gain_ref[:, cols] * norm) - x * pull).astype(bf16)

    for hop in range(depth):
        grads.side_blocks(hop, use_grads)
    proj_out[...] = g_acc[...] * grad_scale

    weights.drain()
    grads.drain()
    for step in range(1, shards):
        vision_to(step).wait_send()
    for step in range(1, groups):
        stat_to(step).wait_send()
    for k in range(len(order)):
        text_to_mate(k).wait_send()
        for yy in far:
            text_to_far(k, yy).wait_send()
    for yy in far + [y]:
        image_to_mate(yy).wait_send()
    for yy in far:
        image_to_far(yy).wait_send()


def live_rows(image_count, groups):
    image_rows = IMG_MAX * PATCH
    row_ids = jnp.arange(groups * image_rows, dtype=jnp.int32)
    owners = row_ids // image_rows
    slot_ids = row_ids % image_rows // PATCH
    owner_match = owners[:, None] == jnp.arange(groups, dtype=jnp.int32)[None, :]
    owner_counts = jnp.sum(jnp.where(owner_match, image_count[None, :], 0), axis=1)
    return (slot_ids < owner_counts)[:, None]


def fused_body(vision_rows, image_count, proj_flat, text_embeds, norm_gain, q_weight, q_grad):
    groups, shards = lax.axis_size("mp"), lax.axis_size("dp")
    model_width, bc = q_weight.shape
    image_rows, enc_width = vision_rows.shape
    text_rows = text_embeds.shape[0]
    shard_k = proj_flat.shape[0] * proj_flat.shape[1] // bc
    chips, depth = groups // CORES, shards // SIDE
    live = live_rows(image_count, groups).astype(jnp.int32)
    grad_scale = 1.0 / float(shards * image_rows) ** 0.5
    f32, bf16 = jnp.float32, jnp.bfloat16
    vmem, dma = pltpu.VMEM, pltpu.SemaphoreType.DMA
    on_chip = pl.BlockSpec(memory_space=pltpu.VMEM)
    anywhere = pl.BlockSpec(memory_space=pl.ANY)
    text_grad, proj_block = pl.pallas_call(
        functools.partial(kernel, shards, groups, grad_scale),
        name="projector_backward",
        out_shape=(
            jax.ShapeDtypeStruct(text_embeds.shape, bf16),
            jax.ShapeDtypeStruct((shard_k, bc), f32),
        ),
        in_specs=[on_chip] * 4 + [anywhere] * 3,
        out_specs=(on_chip, on_chip),
        scratch_shapes=[
            vmem(q_grad.shape, bf16),
            vmem((groups, bc, bc), bf16),
            vmem(text_embeds.shape, bf16),
            vmem((groups, CORES, chips, text_rows, bc), bf16),
            vmem((groups, image_rows, bc), bf16),
            vmem((groups, chips, text_rows, bc), bf16),
            vmem((chips, image_rows, bc), bf16),
            vmem((groups, chips, text_rows, bc), bf16),
            vmem((chips, image_rows, bc), bf16),
            vmem((chips, groups, text_rows, bc), bf16),
            vmem((chips, image_rows, bc), bf16),
            vmem((image_rows, bc), f32),
            vmem((image_rows, bc), f32),
            vmem((shard_k, bc), f32),
            vmem((image_rows, bc), bf16),
            vmem((8, image_rows), f32),
            vmem((groups, 8, image_rows), f32),
            vmem((shards, shard_k, bc), bf16),
            vmem((shards, image_rows, bc), bf16),
            vmem((shards, image_rows, shard_k), bf16),
            dma, dma((groups,)), dma,
            dma((3, depth, CHUNKS)), dma((shards, CHUNKS)),
            dma((3, depth, CHUNKS)), dma((shards, CHUNKS)),
            dma((shards,)), dma((shards,)),
            dma((groups,)), dma((groups,)),
            dma((chips,)), dma((chips,)),
            dma((groups, chips)), dma((chips, groups)),
            dma((chips,)), dma((chips,)),
            dma((groups,)), dma((groups,)),
        ],
        compiler_params=pltpu.CompilerParams(
            collective_id=0, has_side_effects=True, vmem_limit_bytes=56 * 1024 * 1024
        ),
    )(
        proj_flat.reshape(shard_k, bc),
        vision_rows,
        live,
        norm_gain[None, :],
        q_grad,
        q_weight.reshape(groups, bc, bc),
        text_embeds,
    )
    return text_grad, proj_block.reshape(proj_flat.shape)


def norm_back(rows_in, grads, gain):
    inputs = rows_in.astype(jnp.float32)
    inv_rms = lax.rsqrt(jnp.mean(inputs * inputs, axis=-1, keepdims=True) + norm_eps)
    scaled = gain[None, :] * grads
    inner_mean = jnp.mean(scaled * inputs, axis=-1, keepdims=True)
    return inv_rms * scaled - inputs * inv_rms**3 * inner_mean


def general_body(vision_rows, image_count, proj_flat, text_embeds, norm_gain, q_weight, q_grad):
    groups = lax.axis_size("mp")
    member = lax.axis_index("mp")
    shards = lax.axis_size("dp")
    enc_width = vision_rows.shape[1]
    block_cols = q_weight.shape[1]
    model_width = q_weight.shape[0]
    used_count = enc_width * block_cols
    image_rows = IMG_MAX * PATCH
    gathered = lax.all_gather(proj_flat, "dp", axis=0, tiled=True)
    proj_block = gathered.reshape(-1)[:used_count].reshape(enc_width, block_cols)
    embed_cols = jnp.dot(vision_rows, proj_block, preferred_element_type=jnp.float32).astype(
        jnp.bfloat16
    )
    live_group = live_rows(image_count, groups)
    blocks = q_grad.reshape(groups, ROWS_DEV, block_cols)
    image_query = blocks[:, :image_rows].reshape(-1, block_cols)
    text_query = blocks[:, image_rows:].reshape(-1, block_cols)
    image_term = row_term(image_query, q_weight)
    image_norm = lax.psum_scatter(
        image_term.astype(jnp.bfloat16), "mp", scatter_dimension=1, tiled=True
    ).astype(jnp.float32)
    text_norm = lax.psum_scatter(
        row_term(text_query, q_weight).astype(jnp.bfloat16), "mp", scatter_dimension=0, tiled=True
    ).astype(jnp.float32)
    x_cols = embed_cols.astype(jnp.float32)
    gain_cols = lax.dynamic_slice_in_dim(norm_gain, member * block_cols, block_cols)
    scaled = gain_cols[None, :] * image_norm
    squares, inner_sum = lax.psum(
        (jnp.sum(x_cols * x_cols, axis=1), jnp.sum(scaled * x_cols, axis=1)), "mp"
    )
    inv_rms = lax.rsqrt(squares / model_width + norm_eps)[:, None]
    image_input = inv_rms * scaled - x_cols * inv_rms**3 * (inner_sum / model_width)[:, None]
    image_cols = jnp.where(live_group, image_input, 0.0).astype(jnp.bfloat16)
    text_grad = norm_back(text_embeds, text_norm, norm_gain).astype(jnp.bfloat16)
    grad_scale = 1.0 / jnp.sqrt(jnp.float32(shards * groups * image_rows))
    proj_part = (
        lax.dot_general(
            vision_rows, image_cols, (((0,), (0,)), ((), ())), preferred_element_type=jnp.float32
        )
        * grad_scale
    )
    stored_rows = proj_flat.shape[0]
    padded = jnp.pad(proj_part.reshape(-1), (0, shards * stored_rows * 128 - used_count))
    padded = padded.reshape(shards * stored_rows, 128)
    proj_grad = lax.psum_scatter(padded, "dp", scatter_dimension=0, tiled=True)
    return (text_grad, proj_grad)


def body(vision_rows, image_count, proj_flat, text_embeds, norm_gain, q_weight, q_grad):
    groups, shards = lax.axis_size("mp"), lax.axis_size("dp")
    bc = q_weight.shape[1]
    count = proj_flat.shape[0] * proj_flat.shape[1]
    shard_k = count // bc
    fits = (
        count % bc == 0
        and shard_k % 128 == 0
        and shard_k * shards == vision_rows.shape[1]
        and shard_k == vision_rows.shape[0]
        and bc % TILE == 0
        and groups > CORES
        and groups % CORES == 0
        and shards > SIDE
        and shards % SIDE == 0
    )
    run = fused_body if fits else general_body
    return run(vision_rows, image_count, proj_flat, text_embeds, norm_gain, q_weight, q_grad)


def solution(mesh):
    return jax.shard_map(
        body,
        mesh=mesh,
        in_specs=(
            P("dp", None),
            P("dp"),
            P(("dp", "mp"), None),
            P(("dp", "mp"), None),
            P(),
            P(None, "mp"),
            P("dp", "mp"),
        ),
        out_specs=(P(("dp", "mp"), None), P(("dp", "mp"), None)),
        check_vma=False,
    )
```

```python
import functools

import jax
import jax.numpy as jnp
from jax import lax
from jax.experimental import pallas as pl
from jax.experimental.pallas import tpu as pltpu
from jax.sharding import PartitionSpec as P

IMG_MAX = 4
PATCH = 8
ROWS_DEV = 128
CORES = 2
SIDE = 2
CHUNKS = 2
TILE = 256
ROW_STEP = 16

MESH = pl.DeviceIdType.MESH

norm_eps = 1e-05


def row_term(left, weight):
    return lax.dot_general(
        left, weight, (((1,), (1,)), ((), ())), preferred_element_type=jnp.float32
    )


class LineGather:
    def __init__(self, depth, me, member, own, buf, send, recv, turn):
        self.turn_send = turn
        self.depth, self.me, self.member = depth, me, member
        self.z, self.x = me // SIDE, me % SIDE
        self.own, self.buf, self.send, self.recv = own, buf, send, recv
        self.step = buf.shape[1] // CHUNKS

    def rows(self, chunk):
        return pl.ds(chunk * self.step, self.step)

    def copy(self, zz, x, chunk, way, own=False):
        block = zz * SIDE + x
        place = self.buf.at[block, self.rows(chunk)]
        target = (self.me + SIDE, self.me - SIDE, self.z * SIDE + (1 - self.x))[way]
        return pltpu.make_async_remote_copy(
            src_ref=self.own.at[self.rows(chunk)] if own else place,
            dst_ref=place,
            send_sem=self.send.at[way, zz, chunk],
            recv_sem=self.recv.at[block, chunk],
            device_id=(target, self.member),
            device_id_type=MESH,
        )

    def start(self):
        for chunk in range(CHUNKS):
            @pl.when(self.z < self.depth - 1)
            def _():
                self.copy(self.z, self.x, chunk, 0, True).start()

            @pl.when(self.z > 0)
            def _():
                self.copy(self.z, self.x, chunk, 1, True).start()

            self.copy(self.z, self.x, chunk, 2, True).start()

    def turned(self, way):
        block = (self.depth - 1 if way else 0) * SIDE + 1 - self.x
        place = self.buf.at[block, self.rows(CHUNKS - 1)]
        return pltpu.make_async_remote_copy(
            src_ref=place,
            dst_ref=place,
            send_sem=self.turn_send.at[way],
            recv_sem=self.recv.at[block, CHUNKS - 1],
            device_id=(self.me - SIDE if way else self.me + SIDE, self.member),
            device_id_type=MESH,
        )

    def turn(self, hop):
        last = self.depth - 1
        for way, place in ((0, self.z), (1, last - self.z)):
            due = (place == hop) | (place == 0) if hop == 1 else place == hop

            @pl.when(due)
            def _():
                self.turned(way).wait_recv()

                @pl.when(place < last)
                def _():
                    self.turned(way).start()

    def relay(self, hop, chunk):
        below, above = self.z - hop, self.z + hop
        final = chunk == CHUNKS - 1

        @pl.when(below >= 0)
        def _():
            self.copy(below, self.x, chunk, 0).wait_recv()

            @pl.when(self.z < self.depth - 1)
            def _():
                self.copy(below, self.x, chunk, 0).start()

            @pl.when(below > 0 if final else below >= 0)
            def _():
                self.copy(below, self.x, chunk, 2).start()

        @pl.when(above < self.depth)
        def _():
            self.copy(above, self.x, chunk, 1).wait_recv()

            @pl.when(self.z > 0)
            def _():
                self.copy(above, self.x, chunk, 1).start()

            @pl.when(above < self.depth - 1 if final else above < self.depth)
            def _():
                self.copy(above, self.x, chunk, 2).start()

        if final:
            self.turn(hop)

    def line_blocks(self, hop, use):
        for zz in (self.z - hop, self.z + hop):
            @pl.when((zz >= 0) & (zz < self.depth))
            def _():
                use(zz * SIDE + self.x)

    def side_blocks(self, hop, use):
        for zz in (self.z,) if hop == 0 else (self.z - hop, self.z + hop):
            @pl.when((zz >= 0) & (zz < self.depth))
            def _():
                for chunk in range(CHUNKS - 1):
                    self.copy(zz, 1 - self.x, chunk, 2).wait_recv()

                @pl.when((zz > 0) & (zz < self.depth - 1))
                def _():
                    self.copy(zz, 1 - self.x, CHUNKS - 1, 2).wait_recv()

                use(zz * SIDE + 1 - self.x)

    def drain(self):
        for zz in range(self.depth):
            for chunk in range(CHUNKS):
                @pl.when((self.z >= zz) & (self.z < self.depth - 1))
                def _():
                    self.copy(zz, self.x, chunk, 0).wait_send()

                @pl.when((self.z <= zz) & (self.z > 0))
                def _():
                    self.copy(zz, self.x, chunk, 1).wait_send()

                if chunk == CHUNKS - 1 and zz in (0, self.depth - 1):
                    @pl.when(self.z == zz)
                    def _():
                        self.copy(zz, self.x, chunk, 2).wait_send()
                else:
                    self.copy(zz, self.x, chunk, 2).wait_send()
        for way, place in ((0, self.z), (1, self.depth - 1 - self.z)):
            @pl.when(place < self.depth - 1)
            def _():
                self.turned(way).wait_send()


def kernel(
    shards, groups, grad_scale,
    proj_ref, vision_ref, count_ref, gain_ref, q_hbm, w_hbm, text_hbm,
    text_out, proj_out,
    qv, wv, tv, own_text, own_image, mate_text, mate_image, sum_text, sum_image,
    far_text, far_image, scaled_image, x_acc, g_acc, g_own, stat_own, stats,
    w_all, w_flat, g_all, v_all,
    q_sem, w_sem, t_sem, a_send, a_recv, a_turn, c_send, c_recv, c_turn, v_send, v_recv, vm_send, vm_recv,
    mt_send, mt_recv, mi_send, mi_recv, ft_send, ft_recv, fi_send, fi_recv, s_send, s_recv,
):
    me, member = lax.axis_index("dp"), lax.axis_index("mp")
    depth = shards // SIDE
    chips = groups // CORES
    y, core = member // CORES, member % CORES
    mate = y * CORES + 1 - core
    shard_k, block_cols = proj_out.shape
    fold = block_cols // 128
    image_rows = vision_ref.shape[0]
    per_image = image_rows // groups
    rows_dev = qv.shape[0] // groups
    text_rows = rows_dev - per_image
    width = groups * block_cols
    f32, bf16 = jnp.float32, jnp.bfloat16

    far = [lax.rem(y + step, chips) for step in range(1, chips)]
    order = [yy * CORES + lax.rem(core + flip, CORES) for yy in far + [y] for flip in (1, 0)]
    early = len(order) // 2

    q_copy = pltpu.make_async_copy(q_hbm, qv, q_sem)
    q_copy.start()
    w_copies = [pltpu.make_async_copy(w_hbm.at[j], wv.at[j], w_sem.at[k]) for k, j in enumerate(order)]
    for copy in w_copies:
        copy.start()
    t_copy = pltpu.make_async_copy(text_hbm, tv, t_sem)
    t_copy.start()

    barrier = pltpu.get_barrier_semaphore()
    z, x = me // SIDE, me % SIDE

    @pl.when(z > 0)
    def _():
        pl.semaphore_signal(barrier, inc=1, device_id=(me - SIDE, member), device_id_type=MESH)

    @pl.when(z < depth - 1)
    def _():
        pl.semaphore_signal(barrier, inc=1, device_id=(me + SIDE, member), device_id_type=MESH)

    across = z * SIDE + 1 - x
    pl.semaphore_signal(barrier, inc=1, device_id=(across, member), device_id_type=MESH)
    for step in range(1, groups):
        pl.semaphore_signal(
            barrier, inc=1, device_id=(me, lax.rem(member + step, groups)), device_id_type=MESH
        )
    @pl.when((z > 0) & (z < depth - 1))
    def _():
        pl.semaphore_wait(barrier, 2 + groups)

    @pl.when((z == 0) | (z == depth - 1))
    def _():
        pl.semaphore_wait(barrier, 1 + groups)

    weights = LineGather(depth, me, member, proj_ref, w_all, a_send, a_recv, a_turn)
    weights.start()

    def remote(src, dst, send, recv, device):
        return pltpu.make_async_remote_copy(
            src_ref=src, dst_ref=dst, send_sem=send, recv_sem=recv,
            device_id=device, device_id_type=MESH,
        )

    def text_to_mate(k):
        j = order[k]
        return remote(own_text.at[j, 1 - core], mate_text.at[j], mt_send.at[j], mt_recv.at[j], (me, mate))

    def image_to_mate(yy):
        return remote(
            own_image.at[yy * CORES + 1 - core], mate_image.at[yy],
            mi_send.at[yy], mi_recv.at[yy], (me, mate),
        )

    def text_to_far(k, yy):
        j = order[k]
        return remote(
            sum_text.at[j, yy], far_text.at[y, j], ft_send.at[j, yy], ft_recv.at[y, j],
            (me, yy * CORES + core),
        )

    def text_from_far(k, yy):
        j = order[k]
        return remote(
            sum_text.at[j, yy], far_text.at[yy, j], ft_send.at[j, yy], ft_recv.at[yy, j],
            (me, yy * CORES + core),
        )

    def image_to_far(yy):
        return remote(
            sum_image.at[yy], far_image.at[y], fi_send.at[yy], fi_recv.at[y], (me, yy * CORES + core)
        )

    def image_from_far(yy):
        return remote(
            sum_image.at[yy], far_image.at[yy], fi_send.at[yy], fi_recv.at[yy], (me, yy * CORES + core)
        )

    def multiply(k):
        j = order[k]
        w_copies[k].wait()

        @pl.loop(0, block_cols // TILE)
        def _(n):
            cols = pl.ds(pl.multiple_of(n * TILE, TILE), TILE)
            term = row_term(qv[...], wv[j, cols, :]).astype(bf16)
            for g in range(groups):
                base = g * rows_dev
                own_image[j, pl.ds(g * per_image, per_image), cols] = term[base : base + per_image]
                own_text[j, g % CORES, g // CORES, :, cols] = term[base + per_image : base + rows_dev]

        text_to_mate(k).start()

    def add_image(yy):
        image_to_mate(yy).wait_recv()

        @pl.loop(0, image_rows // ROW_STEP)
        def _(n):
            rows = pl.ds(pl.multiple_of(n * ROW_STEP, ROW_STEP), ROW_STEP)
            total = own_image[yy * CORES + core, rows].astype(f32) + mate_image[yy, rows].astype(f32)
            sum_image[yy, rows] = total.astype(bf16)

    def add_text(k):
        j = order[k]
        text_to_mate(k).wait_recv()
        for yy in far:
            @pl.loop(0, text_rows // ROW_STEP)
            def _(n):
                rows = pl.ds(pl.multiple_of(n * ROW_STEP, ROW_STEP), ROW_STEP)
                total = own_text[j, core, yy, rows].astype(f32) + mate_text[j, yy, rows].astype(f32)
                sum_text[j, yy, rows] = total.astype(bf16)

    def send_text(k):
        for yy in far:
            text_to_far(k, yy).start()

    q_copy.wait()
    for k in range(early):
        multiply(k)
        if k % CORES == 0:
            image_to_mate(far[k // CORES]).start() if k // CORES < len(far) else None
    for yy in far[: early // CORES]:
        add_image(yy)
        image_to_far(yy).start()
    weights.relay(1, 0)
    for k in range(early):
        add_text(k)
        send_text(k)
    for chunk in range(1, CHUNKS):
        weights.relay(1, chunk)
    for k in range(early, len(order)):
        multiply(k)
        if k % CORES == 0:
            image_to_mate((far + [y])[k // CORES]).start()
        if 2 < depth and k - early < CHUNKS:
            weights.relay(2, k - early)
    for yy in far[early // CORES :]:
        add_image(yy)
        image_to_far(yy).start()
    for chunk in range(len(order) - early, CHUNKS):
        weights.relay(2, chunk)

    def wide(shard):
        w_flat[...] = shard[...].astype(f32)
        parts = [w_flat[pl.ds(c, shard_k, stride=fold), :] for c in range(fold)]
        return jnp.concatenate(parts, axis=1).astype(bf16)

    def use_weights(block):
        cols = pl.ds(pl.multiple_of(block * shard_k, shard_k), shard_k)
        x_acc[...] += jnp.dot(vision_ref[:, cols], wide(w_all.at[block]), preferred_element_type=f32)

    own_cols = pl.ds(pl.multiple_of(me * shard_k, shard_k), shard_k)
    x_acc[...] = jnp.dot(vision_ref[:, own_cols], wide(proj_ref), preferred_element_type=f32)
    weights.line_blocks(1, use_weights)
    for hop in range(3, depth):
        for chunk in range(CHUNKS):
            weights.relay(hop, chunk)
    for hop in range(2, depth):
        weights.line_blocks(hop, use_weights)

    half = image_rows // CORES
    my_half = pl.ds(pl.multiple_of(core * half, half), half)
    mate_half = pl.ds(pl.multiple_of((1 - core) * half, half), half)

    def vision_to(step):
        target = lax.rem(me + step, shards)
        cols = pl.ds(pl.multiple_of(target * shard_k, shard_k), shard_k)
        return remote(
            vision_ref.at[my_half, cols], v_all.at[me, my_half],
            v_send.at[target], v_recv.at[me], (target, member),
        )

    def vision_from(step):
        source = lax.rem(me + step, shards)
        cols = pl.ds(pl.multiple_of(source * shard_k, shard_k), shard_k)
        return remote(
            vision_ref.at[my_half, cols], v_all.at[source, my_half],
            v_send.at[source], v_recv.at[source], (source, member),
        )

    def vision_to_mate(source):
        place = v_all.at[source, my_half]
        return remote(place, place, vm_send.at[source], vm_recv.at[source], (me, mate))

    def vision_from_mate(source):
        place = v_all.at[source, mate_half]
        return remote(place, place, vm_send.at[source], vm_recv.at[source], (me, mate))

    image_to_mate(y).wait_recv()
    for yy in far:
        image_from_far(yy).wait_recv()
    member_cols = pl.ds(pl.multiple_of(member * block_cols, block_cols), block_cols)

    @pl.loop(0, image_rows // ROW_STEP)
    def _(n):
        rows = pl.ds(pl.multiple_of(n * ROW_STEP, ROW_STEP), ROW_STEP)
        total = own_image[member, rows].astype(f32) + mate_image[y, rows].astype(f32)
        for yy in far:
            total = total + far_image[yy, rows].astype(f32)
        scaled_image[rows] = gain_ref[:, member_cols] * total

    for k in range(early, len(order)):
        add_text(k)
    for hop in range(depth):
        weights.side_blocks(hop, use_weights)
    for step in range(1, shards):
        vision_to(step).start()

    @pl.loop(0, image_rows // ROW_STEP)
    def _(n):
        rows = pl.ds(pl.multiple_of(n * ROW_STEP, ROW_STEP), ROW_STEP)
        x = x_acc[rows].astype(bf16).astype(f32)
        x_acc[rows] = x
        squares = jnp.sum(x * x, axis=1, keepdims=True)
        inner = jnp.sum(x * scaled_image[rows], axis=1, keepdims=True)
        lane = lax.broadcasted_iota(jnp.int32, (ROW_STEP, 128), 1)
        g_acc[rows, pl.ds(0, 128)] = jnp.where(lane == 0, squares, inner)

    stat_own[...] = g_acc[:, 0:128].T[0:8]

    def stat_to(step):
        target = lax.rem(member + step, groups)
        return remote(stat_own, stats.at[member], s_send.at[target], s_recv.at[member], (me, target))

    def stat_from(step):
        source = lax.rem(member + step, groups)
        return remote(stat_own, stats.at[source], s_send.at[source], s_recv.at[source], (me, source))

    for step in range(1, groups):
        stat_to(step).start()
    for k in range(early, len(order)):
        send_text(k)
    total = stat_own[...]
    for step in range(1, groups):
        stat_from(step).wait_recv()
        total = total + stats[lax.rem(member + step, groups)]
    spread = jnp.concatenate([total] * 16, axis=0).T
    inv_all = lax.rsqrt(spread[:, 0:1] / width + norm_eps)
    g_acc[:, 0:128] = jnp.broadcast_to(inv_all, (image_rows, 128))
    g_acc[:, 128:256] = jnp.broadcast_to(inv_all**3 * (spread[:, 1:2] / width), (image_rows, 128))

    for g in range(groups):
        held = count_ref[g] * PATCH

        @pl.loop(0, per_image // ROW_STEP)
        def _(n):
            first = n * ROW_STEP
            rows = pl.ds(pl.multiple_of(g * per_image + first, ROW_STEP), ROW_STEP)
            inv, pull = g_acc[rows, pl.ds(0, 1)], g_acc[rows, pl.ds(128, 1)]
            grad = inv * scaled_image[rows] - x_acc[rows] * pull
            slots = first + lax.broadcasted_iota(jnp.int32, (ROW_STEP, block_cols), 0)
            g_own[rows] = jnp.where(slots < held, grad, 0.0).astype(bf16)

    grads = LineGather(depth, me, member, g_own, g_all, c_send, c_recv, c_turn)
    grads.start()

    def vision_term(left, right):
        return lax.dot_general(left, right, (((0,), (0,)), ((), ())), preferred_element_type=f32)

    def use_grads(block):
        vision_from_mate(block).wait_recv()
        g_acc[...] += vision_term(v_all[block], g_all[block])

    g_acc[...] = vision_term(vision_ref[:, own_cols], g_own[...])
    for step in range(1, shards):
        vision_from(step).wait_recv()
        vision_to_mate(lax.rem(me + step, shards)).start()
    for hop in range(1, depth):
        for chunk in range(CHUNKS):
            grads.relay(hop, chunk)
        if hop < depth - 1:
            grads.line_blocks(hop, use_grads)
    grads.line_blocks(depth - 1, use_grads)

    for k in range(len(order)):
        for yy in far:
            text_from_far(k, yy).wait_recv()
    t_copy.wait()

    @pl.loop(0, text_rows // ROW_STEP)
    def _(n):
        rows = pl.ds(pl.multiple_of(n * ROW_STEP, ROW_STEP), ROW_STEP)
        squares = jnp.zeros((ROW_STEP, 1), f32)
        inner = jnp.zeros((ROW_STEP, 1), f32)
        for j in range(groups):
            cols = pl.ds(j * block_cols, block_cols)
            x = tv[rows, cols].astype(f32)
            norm = own_text[j, core, y, rows].astype(f32) + mate_text[j, y, rows].astype(f32)
            for yy in far:
                norm = norm + far_text[yy, j, rows].astype(f32)
            scaled = gain_ref[:, cols] * norm
            squares += jnp.sum(x * x, axis=1, keepdims=True)
            inner += jnp.sum(x * scaled, axis=1, keepdims=True)
        inv = lax.rsqrt(squares / width + norm_eps)
        pull = inv**3 * (inner / width)
        for j in range(groups):
            cols = pl.ds(j * block_cols, block_cols)
            x = tv[rows, cols].astype(f32)
            norm = own_text[j, core, y, rows].astype(f32) + mate_text[j, y, rows].astype(f32)
            for yy in far:
                norm = norm + far_text[yy, j, rows].astype(f32)
            text_out[rows, cols] = (inv * (gain_ref[:, cols] * norm) - x * pull).astype(bf16)

    for hop in range(depth):
        grads.side_blocks(hop, use_grads)
    proj_out[...] = g_acc[...] * grad_scale

    weights.drain()
    grads.drain()
    for step in range(1, shards):
        vision_to(step).wait_send()
        vision_to_mate(lax.rem(me + step, shards)).wait_send()
    for step in range(1, groups):
        stat_to(step).wait_send()
    for k in range(len(order)):
        text_to_mate(k).wait_send()
        for yy in far:
            text_to_far(k, yy).wait_send()
    for yy in far + [y]:
        image_to_mate(yy).wait_send()
    for yy in far:
        image_to_far(yy).wait_send()


def live_rows(image_count, groups):
    image_rows = IMG_MAX * PATCH
    row_ids = jnp.arange(groups * image_rows, dtype=jnp.int32)
    owners = row_ids // image_rows
    slot_ids = row_ids % image_rows // PATCH
    owner_match = owners[:, None] == jnp.arange(groups, dtype=jnp.int32)[None, :]
    owner_counts = jnp.sum(jnp.where(owner_match, image_count[None, :], 0), axis=1)
    return (slot_ids < owner_counts)[:, None]


def fused_body(vision_rows, image_count, proj_flat, text_embeds, norm_gain, q_weight, q_grad):
    groups, shards = lax.axis_size("mp"), lax.axis_size("dp")
    model_width, bc = q_weight.shape
    image_rows, enc_width = vision_rows.shape
    text_rows = text_embeds.shape[0]
    shard_k = proj_flat.shape[0] * proj_flat.shape[1] // bc
    chips, depth = groups // CORES, shards // SIDE
    grad_scale = 1.0 / float(shards * image_rows) ** 0.5
    f32, bf16 = jnp.float32, jnp.bfloat16
    vmem, dma = pltpu.VMEM, pltpu.SemaphoreType.DMA
    on_chip = pl.BlockSpec(memory_space=pltpu.VMEM)
    scalars = pl.BlockSpec(memory_space=pltpu.SMEM)
    anywhere = pl.BlockSpec(memory_space=pl.ANY)
    text_grad, proj_block = pl.pallas_call(
        functools.partial(kernel, shards, groups, grad_scale),
        name="projector_backward",
        out_shape=(
            jax.ShapeDtypeStruct(text_embeds.shape, bf16),
            jax.ShapeDtypeStruct((shard_k, bc), f32),
        ),
        in_specs=[on_chip, on_chip, scalars, on_chip] + [anywhere] * 3,
        out_specs=(on_chip, on_chip),
        scratch_shapes=[
            vmem(q_grad.shape, bf16),
            vmem((groups, bc, bc), bf16),
            vmem(text_embeds.shape, bf16),
            vmem((groups, CORES, chips, text_rows, bc), bf16),
            vmem((groups, image_rows, bc), bf16),
            vmem((groups, chips, text_rows, bc), bf16),
            vmem((chips, image_rows, bc), bf16),
            vmem((groups, chips, text_rows, bc), bf16),
            vmem((chips, image_rows, bc), bf16),
            vmem((chips, groups, text_rows, bc), bf16),
            vmem((chips, image_rows, bc), bf16),
            vmem((image_rows, bc), f32),
            vmem((image_rows, bc), f32),
            vmem((shard_k, bc), f32),
            vmem((image_rows, bc), bf16),
            vmem((8, image_rows), f32),
            vmem((groups, 8, image_rows), f32),
            vmem((shards,) + proj_flat.shape, bf16),
            vmem(proj_flat.shape, f32),
            vmem((shards, image_rows, bc), bf16),
            vmem((shards, image_rows, shard_k), bf16),
            dma, dma((groups,)), dma,
            dma((3, depth, CHUNKS)), dma((shards, CHUNKS)), dma((2,)),
            dma((3, depth, CHUNKS)), dma((shards, CHUNKS)), dma((2,)),
            dma((shards,)), dma((shards,)), dma((shards,)), dma((shards,)),
            dma((groups,)), dma((groups,)),
            dma((chips,)), dma((chips,)),
            dma((groups, chips)), dma((chips, groups)),
            dma((chips,)), dma((chips,)),
            dma((groups,)), dma((groups,)),
        ],
        compiler_params=pltpu.CompilerParams(
            collective_id=0, has_side_effects=True, vmem_limit_bytes=56 * 1024 * 1024
        ),
    )(
        proj_flat,
        vision_rows,
        image_count,
        norm_gain[None, :],
        q_grad,
        q_weight.reshape(groups, bc, bc),
        text_embeds,
    )
    return text_grad, proj_block.reshape(proj_flat.shape)


def norm_back(rows_in, grads, gain):
    inputs = rows_in.astype(jnp.float32)
    inv_rms = lax.rsqrt(jnp.mean(inputs * inputs, axis=-1, keepdims=True) + norm_eps)
    scaled = gain[None, :] * grads
    inner_mean = jnp.mean(scaled * inputs, axis=-1, keepdims=True)
    return inv_rms * scaled - inputs * inv_rms**3 * inner_mean


def general_body(vision_rows, image_count, proj_flat, text_embeds, norm_gain, q_weight, q_grad):
    groups = lax.axis_size("mp")
    member = lax.axis_index("mp")
    shards = lax.axis_size("dp")
    enc_width = vision_rows.shape[1]
    block_cols = q_weight.shape[1]
    model_width = q_weight.shape[0]
    used_count = enc_width * block_cols
    image_rows = IMG_MAX * PATCH
    gathered = lax.all_gather(proj_flat, "dp", axis=0, tiled=True)
    proj_block = gathered.reshape(-1)[:used_count].reshape(enc_width, block_cols)
    embed_cols = jnp.dot(vision_rows, proj_block, preferred_element_type=jnp.float32).astype(
        jnp.bfloat16
    )
    live_group = live_rows(image_count, groups)
    blocks = q_grad.reshape(groups, ROWS_DEV, block_cols)
    image_query = blocks[:, :image_rows].reshape(-1, block_cols)
    text_query = blocks[:, image_rows:].reshape(-1, block_cols)
    image_term = row_term(image_query, q_weight)
    image_norm = lax.psum_scatter(
        image_term.astype(jnp.bfloat16), "mp", scatter_dimension=1, tiled=True
    ).astype(jnp.float32)
    text_norm = lax.psum_scatter(
        row_term(text_query, q_weight).astype(jnp.bfloat16), "mp", scatter_dimension=0, tiled=True
    ).astype(jnp.float32)
    x_cols = embed_cols.astype(jnp.float32)
    gain_cols = lax.dynamic_slice_in_dim(norm_gain, member * block_cols, block_cols)
    scaled = gain_cols[None, :] * image_norm
    squares, inner_sum = lax.psum(
        (jnp.sum(x_cols * x_cols, axis=1), jnp.sum(scaled * x_cols, axis=1)), "mp"
    )
    inv_rms = lax.rsqrt(squares / model_width + norm_eps)[:, None]
    image_input = inv_rms * scaled - x_cols * inv_rms**3 * (inner_sum / model_width)[:, None]
    image_cols = jnp.where(live_group, image_input, 0.0).astype(jnp.bfloat16)
    text_grad = norm_back(text_embeds, text_norm, norm_gain).astype(jnp.bfloat16)
    grad_scale = 1.0 / jnp.sqrt(jnp.float32(shards * groups * image_rows))
    proj_part = (
        lax.dot_general(
            vision_rows, image_cols, (((0,), (0,)), ((), ())), preferred_element_type=jnp.float32
        )
        * grad_scale
    )
    stored_rows = proj_flat.shape[0]
    padded = jnp.pad(proj_part.reshape(-1), (0, shards * stored_rows * 128 - used_count))
    padded = padded.reshape(shards * stored_rows, 128)
    proj_grad = lax.psum_scatter(padded, "dp", scatter_dimension=0, tiled=True)
    return (text_grad, proj_grad)


def body(vision_rows, image_count, proj_flat, text_embeds, norm_gain, q_weight, q_grad):
    groups, shards = lax.axis_size("mp"), lax.axis_size("dp")
    bc = q_weight.shape[1]
    count = proj_flat.shape[0] * proj_flat.shape[1]
    shard_k = count // bc
    fits = (
        count % bc == 0
        and shard_k % 128 == 0
        and shard_k * shards == vision_rows.shape[1]
        and shard_k == vision_rows.shape[0]
        and bc % TILE == 0
        and groups > CORES
        and groups % CORES == 0
        and vision_rows.shape[0] // groups % ROW_STEP == 0
        and text_embeds.shape[0] % ROW_STEP == 0
        and shards > SIDE
        and shards % SIDE == 0
    )
    run = fused_body if fits else general_body
    return run(vision_rows, image_count, proj_flat, text_embeds, norm_gain, q_weight, q_grad)


def solution(mesh):
    return jax.shard_map(
        body,
        mesh=mesh,
        in_specs=(
            P("dp", None),
            P("dp"),
            P(("dp", "mp"), None),
            P(("dp", "mp"), None),
            P(),
            P(None, "mp"),
            P("dp", "mp"),
        ),
        out_specs=(P(("dp", "mp"), None), P(("dp", "mp"), None)),
        check_vma=False,
    )
```

```python
import functools

import jax
import jax.numpy as jnp
from jax import lax
from jax.experimental import pallas as pl
from jax.experimental.pallas import tpu as pltpu
from jax.sharding import PartitionSpec as P

IMG_MAX = 4
PATCH = 8
ROWS_DEV = 128
CORES = 2
SIDE = 2
CHUNKS = 4
TURNED = 1
PIECES = 2
TILE = 256
ROW_STEP = 16

MESH = pl.DeviceIdType.MESH

norm_eps = 1e-05


def row_term(left, weight):
    return lax.dot_general(
        left, weight, (((1,), (1,)), ((), ())), preferred_element_type=jnp.float32
    )


class LineGather:
    def __init__(self, depth, me, member, own, buf, send, recv, turn):
        self.turn_send = turn
        self.depth, self.me, self.member = depth, me, member
        self.z, self.x = me // SIDE, me % SIDE
        self.own, self.buf, self.send, self.recv = own, buf, send, recv
        self.step = buf.shape[1] // CHUNKS

    def rows(self, chunk):
        return pl.ds(chunk * self.step, self.step)

    def copy(self, zz, x, chunk, way, own=False):
        block = zz * SIDE + x
        place = self.buf.at[block, self.rows(chunk)]
        target = (self.me + SIDE, self.me - SIDE, self.z * SIDE + (1 - self.x))[way]
        return pltpu.make_async_remote_copy(
            src_ref=self.own.at[self.rows(chunk)] if own else place,
            dst_ref=place,
            send_sem=self.send.at[way, zz, chunk],
            recv_sem=self.recv.at[block, chunk],
            device_id=(target, self.member),
            device_id_type=MESH,
        )

    def start(self):
        for chunk in range(CHUNKS):
            @pl.when(self.z < self.depth - 1)
            def _():
                self.copy(self.z, self.x, chunk, 0, True).start()

            @pl.when(self.z > 0)
            def _():
                self.copy(self.z, self.x, chunk, 1, True).start()

            self.copy(self.z, self.x, chunk, 2, True).start()

    def turned(self, way, chunk):
        block = (self.depth - 1 if way else 0) * SIDE + 1 - self.x
        place = self.buf.at[block, self.rows(chunk)]
        return pltpu.make_async_remote_copy(
            src_ref=place,
            dst_ref=place,
            send_sem=self.turn_send.at[way, chunk],
            recv_sem=self.recv.at[block, chunk],
            device_id=(self.me - SIDE if way else self.me + SIDE, self.member),
            device_id_type=MESH,
        )

    def turn(self, hop):
        last = self.depth - 1
        for way, place in ((0, self.z), (1, last - self.z)):
            due = (place == hop) | (place == 0) if hop == 1 else place == hop

            @pl.when(due)
            def _():
                for chunk in range(CHUNKS - TURNED, CHUNKS):
                    self.turned(way, chunk).wait_recv()

                    @pl.when(place < last)
                    def _():
                        self.turned(way, chunk).start()

    def relay(self, hop, chunk):
        below, above = self.z - hop, self.z + hop
        final = chunk >= CHUNKS - TURNED

        @pl.when(below >= 0)
        def _():
            self.copy(below, self.x, chunk, 0).wait_recv()

            @pl.when(self.z < self.depth - 1)
            def _():
                self.copy(below, self.x, chunk, 0).start()

            @pl.when(below > 0 if final else below >= 0)
            def _():
                self.copy(below, self.x, chunk, 2).start()

        @pl.when(above < self.depth)
        def _():
            self.copy(above, self.x, chunk, 1).wait_recv()

            @pl.when(self.z > 0)
            def _():
                self.copy(above, self.x, chunk, 1).start()

            @pl.when(above < self.depth - 1 if final else above < self.depth)
            def _():
                self.copy(above, self.x, chunk, 2).start()

        if chunk == CHUNKS - 1:
            self.turn(hop)

    def line_blocks(self, hop, use):
        for zz in (self.z - hop, self.z + hop):
            @pl.when((zz >= 0) & (zz < self.depth))
            def _():
                use(zz * SIDE + self.x)

    def side_blocks(self, hop, use):
        for zz in (self.z,) if hop == 0 else (self.z - hop, self.z + hop):
            @pl.when((zz >= 0) & (zz < self.depth))
            def _():
                for chunk in range(CHUNKS - TURNED):
                    self.copy(zz, 1 - self.x, chunk, 2).wait_recv()

                @pl.when((zz > 0) & (zz < self.depth - 1))
                def _():
                    for chunk in range(CHUNKS - TURNED, CHUNKS):
                        self.copy(zz, 1 - self.x, chunk, 2).wait_recv()

                use(zz * SIDE + 1 - self.x)

    def drain(self):
        for zz in range(self.depth):
            for chunk in range(CHUNKS):
                @pl.when((self.z >= zz) & (self.z < self.depth - 1))
                def _():
                    self.copy(zz, self.x, chunk, 0).wait_send()

                @pl.when((self.z <= zz) & (self.z > 0))
                def _():
                    self.copy(zz, self.x, chunk, 1).wait_send()

                if chunk >= CHUNKS - TURNED and zz in (0, self.depth - 1):
                    @pl.when(self.z == zz)
                    def _():
                        self.copy(zz, self.x, chunk, 2).wait_send()
                else:
                    self.copy(zz, self.x, chunk, 2).wait_send()
        for way, place in ((0, self.z), (1, self.depth - 1 - self.z)):
            @pl.when(place < self.depth - 1)
            def _():
                for chunk in range(CHUNKS - TURNED, CHUNKS):
                    self.turned(way, chunk).wait_send()


def kernel(
    shards, groups, grad_scale,
    proj_ref, vision_ref, count_ref, gain_ref, q_hbm, w_hbm, text_hbm,
    text_out, proj_out,
    qv, wv, tv, own_text, own_image, mate_text, mate_image, sum_text, sum_image,
    far_text, far_image, scaled_image, x_acc, g_acc, g_own, stat_own, stats,
    w_all, w_flat, g_all, v_all,
    q_sem, w_sem, t_sem, a_send, a_recv, a_turn, c_send, c_recv, c_turn, v_send, v_recv, vm_send, vm_recv,
    mt_send, mt_recv, mi_send, mi_recv, ft_send, ft_recv, fi_send, fi_recv, s_send, s_recv,
):
    me, member = lax.axis_index("dp"), lax.axis_index("mp")
    depth = shards // SIDE
    chips = groups // CORES
    y, core = member // CORES, member % CORES
    mate = y * CORES + 1 - core
    shard_k, block_cols = g_acc.shape
    fold = block_cols // 128
    image_rows = vision_ref.shape[0]
    per_image = image_rows // groups
    rows_dev = qv.shape[0] // groups
    text_rows = rows_dev - per_image
    width = groups * block_cols
    f32, bf16 = jnp.float32, jnp.bfloat16

    far = [lax.rem(y + step, chips) for step in range(1, chips)]
    order = [yy * CORES + lax.rem(core + flip, CORES) for yy in far + [y] for flip in (1, 0)]
    early = len(order) // 2

    q_copy = pltpu.make_async_copy(q_hbm, qv, q_sem)
    q_copy.start()
    w_copies = [pltpu.make_async_copy(w_hbm.at[j], wv.at[j], w_sem.at[k]) for k, j in enumerate(order)]
    for copy in w_copies:
        copy.start()
    t_copy = pltpu.make_async_copy(text_hbm, tv, t_sem)
    t_copy.start()

    barrier = pltpu.get_barrier_semaphore()
    z, x = me // SIDE, me % SIDE

    @pl.when(z > 0)
    def _():
        pl.semaphore_signal(barrier, inc=1, device_id=(me - SIDE, member), device_id_type=MESH)

    @pl.when(z < depth - 1)
    def _():
        pl.semaphore_signal(barrier, inc=1, device_id=(me + SIDE, member), device_id_type=MESH)

    across = z * SIDE + 1 - x
    pl.semaphore_signal(barrier, inc=1, device_id=(across, member), device_id_type=MESH)
    for step in range(1, groups):
        pl.semaphore_signal(
            barrier, inc=1, device_id=(me, lax.rem(member + step, groups)), device_id_type=MESH
        )
    @pl.when((z > 0) & (z < depth - 1))
    def _():
        pl.semaphore_wait(barrier, 2 + groups)

    @pl.when((z == 0) | (z == depth - 1))
    def _():
        pl.semaphore_wait(barrier, 1 + groups)

    weights = LineGather(depth, me, member, proj_ref, w_all, a_send, a_recv, a_turn)
    weights.start()

    def remote(src, dst, send, recv, device):
        return pltpu.make_async_remote_copy(
            src_ref=src, dst_ref=dst, send_sem=send, recv_sem=recv,
            device_id=device, device_id_type=MESH,
        )

    def text_to_mate(k):
        j = order[k]
        return remote(own_text.at[j, 1 - core], mate_text.at[j], mt_send.at[j], mt_recv.at[j], (me, mate))

    def image_to_mate(yy):
        return remote(
            own_image.at[yy * CORES + 1 - core], mate_image.at[yy],
            mi_send.at[yy], mi_recv.at[yy], (me, mate),
        )

    def text_to_far(k, yy):
        j = order[k]
        return remote(
            sum_text.at[j, yy], far_text.at[y, j], ft_send.at[j, yy], ft_recv.at[y, j],
            (me, yy * CORES + core),
        )

    def text_from_far(k, yy):
        j = order[k]
        return remote(
            sum_text.at[j, yy], far_text.at[yy, j], ft_send.at[j, yy], ft_recv.at[yy, j],
            (me, yy * CORES + core),
        )

    def image_to_far(yy):
        return remote(
            sum_image.at[yy], far_image.at[y], fi_send.at[yy], fi_recv.at[y], (me, yy * CORES + core)
        )

    def image_from_far(yy):
        return remote(
            sum_image.at[yy], far_image.at[yy], fi_send.at[yy], fi_recv.at[yy], (me, yy * CORES + core)
        )

    def multiply(k):
        j = order[k]
        w_copies[k].wait()

        @pl.loop(0, block_cols // TILE)
        def _(n):
            cols = pl.ds(pl.multiple_of(n * TILE, TILE), TILE)
            term = row_term(qv[...], wv[j, cols, :]).astype(bf16)
            for g in range(groups):
                base = g * rows_dev
                own_image[j, pl.ds(g * per_image, per_image), cols] = term[base : base + per_image]
                own_text[j, g % CORES, g // CORES, :, cols] = term[base + per_image : base + rows_dev]

        text_to_mate(k).start()

    def add_image(yy):
        image_to_mate(yy).wait_recv()

        @pl.loop(0, image_rows // ROW_STEP)
        def _(n):
            rows = pl.ds(pl.multiple_of(n * ROW_STEP, ROW_STEP), ROW_STEP)
            total = own_image[yy * CORES + core, rows].astype(f32) + mate_image[yy, rows].astype(f32)
            sum_image[yy, rows] = total.astype(bf16)

    def add_text(k):
        j = order[k]
        text_to_mate(k).wait_recv()
        for yy in far:
            @pl.loop(0, text_rows // ROW_STEP)
            def _(n):
                rows = pl.ds(pl.multiple_of(n * ROW_STEP, ROW_STEP), ROW_STEP)
                total = own_text[j, core, yy, rows].astype(f32) + mate_text[j, yy, rows].astype(f32)
                sum_text[j, yy, rows] = total.astype(bf16)

    def send_text(k):
        for yy in far:
            text_to_far(k, yy).start()

    q_copy.wait()
    for k in range(early):
        multiply(k)
        if k % CORES == 0:
            image_to_mate(far[k // CORES]).start() if k // CORES < len(far) else None
    for yy in far[: early // CORES]:
        add_image(yy)
        image_to_far(yy).start()
    weights.relay(1, 0)
    for k in range(early):
        add_text(k)
        send_text(k)
    for chunk in range(1, CHUNKS):
        weights.relay(1, chunk)
    for k in range(early, len(order)):
        multiply(k)
        if k % CORES == 0:
            image_to_mate((far + [y])[k // CORES]).start()
        if 2 < depth and k - early < CHUNKS:
            weights.relay(2, k - early)
    for yy in far[early // CORES :]:
        add_image(yy)
        image_to_far(yy).start()
    for chunk in range(len(order) - early, CHUNKS):
        weights.relay(2, chunk)

    def wide(shard):
        w_flat[...] = shard[...].astype(f32)
        parts = [w_flat[pl.ds(c, shard_k, stride=fold), :] for c in range(fold)]
        return jnp.concatenate(parts, axis=1).astype(bf16)

    def use_weights(block):
        cols = pl.ds(pl.multiple_of(block * shard_k, shard_k), shard_k)
        x_acc[...] += jnp.dot(vision_ref[:, cols], wide(w_all.at[block]), preferred_element_type=f32)

    own_cols = pl.ds(pl.multiple_of(me * shard_k, shard_k), shard_k)
    x_acc[...] = jnp.dot(vision_ref[:, own_cols], wide(proj_ref), preferred_element_type=f32)
    weights.line_blocks(1, use_weights)
    for hop in range(3, depth):
        for chunk in range(CHUNKS):
            weights.relay(hop, chunk)
    for hop in range(2, depth):
        weights.line_blocks(hop, use_weights)

    half = image_rows // CORES
    my_half = pl.ds(pl.multiple_of(core * half, half), half)
    mate_half = pl.ds(pl.multiple_of((1 - core) * half, half), half)

    def vision_to(step):
        target = lax.rem(me + step, shards)
        cols = pl.ds(pl.multiple_of(target * shard_k, shard_k), shard_k)
        return remote(
            vision_ref.at[my_half, cols], v_all.at[me, my_half],
            v_send.at[target], v_recv.at[me], (target, member),
        )

    def vision_from(step):
        source = lax.rem(me + step, shards)
        cols = pl.ds(pl.multiple_of(source * shard_k, shard_k), shard_k)
        return remote(
            vision_ref.at[my_half, cols], v_all.at[source, my_half],
            v_send.at[source], v_recv.at[source], (source, member),
        )

    def vision_to_mate(source):
        place = v_all.at[source, my_half]
        return remote(place, place, vm_send.at[source], vm_recv.at[source], (me, mate))

    def vision_from_mate(source):
        place = v_all.at[source, mate_half]
        return remote(place, place, vm_send.at[source], vm_recv.at[source], (me, mate))

    image_to_mate(y).wait_recv()
    for yy in far:
        image_from_far(yy).wait_recv()
    member_cols = pl.ds(pl.multiple_of(member * block_cols, block_cols), block_cols)

    @pl.loop(0, image_rows // ROW_STEP)
    def _(n):
        rows = pl.ds(pl.multiple_of(n * ROW_STEP, ROW_STEP), ROW_STEP)
        total = own_image[member, rows].astype(f32) + mate_image[y, rows].astype(f32)
        for yy in far:
            total = total + far_image[yy, rows].astype(f32)
        scaled_image[rows] = gain_ref[:, member_cols] * total

    for k in range(early, len(order)):
        add_text(k)
    for hop in range(depth):
        weights.side_blocks(hop, use_weights)
    for step in range(1, shards):
        vision_to(step).start()

    @pl.loop(0, image_rows // ROW_STEP)
    def _(n):
        rows = pl.ds(pl.multiple_of(n * ROW_STEP, ROW_STEP), ROW_STEP)
        x = x_acc[rows].astype(bf16).astype(f32)
        x_acc[rows] = x
        squares = jnp.sum(x * x, axis=1, keepdims=True)
        inner = jnp.sum(x * scaled_image[rows], axis=1, keepdims=True)
        lane = lax.broadcasted_iota(jnp.int32, (ROW_STEP, 128), 1)
        g_acc[rows, pl.ds(0, 128)] = jnp.where(lane == 0, squares, inner)

    stat_own[...] = g_acc[:, 0:128].T[0:8]

    def stat_to(step):
        target = lax.rem(member + step, groups)
        return remote(stat_own, stats.at[member], s_send.at[target], s_recv.at[member], (me, target))

    def stat_from(step):
        source = lax.rem(member + step, groups)
        return remote(stat_own, stats.at[source], s_send.at[source], s_recv.at[source], (me, source))

    for step in range(1, groups):
        stat_to(step).start()
    for k in range(early, len(order)):
        send_text(k)
    total = stat_own[...]
    for step in range(1, groups):
        stat_from(step).wait_recv()
        total = total + stats[lax.rem(member + step, groups)]
    spread = jnp.concatenate([total] * 16, axis=0).T
    inv_all = lax.rsqrt(spread[:, 0:1] / width + norm_eps)
    g_acc[:, 0:128] = jnp.broadcast_to(inv_all, (image_rows, 128))
    g_acc[:, 128:256] = jnp.broadcast_to(inv_all**3 * (spread[:, 1:2] / width), (image_rows, 128))

    for g in range(groups):
        held = count_ref[g] * PATCH

        @pl.loop(0, per_image // ROW_STEP)
        def _(n):
            first = n * ROW_STEP
            rows = pl.ds(pl.multiple_of(g * per_image + first, ROW_STEP), ROW_STEP)
            inv, pull = g_acc[rows, pl.ds(0, 1)], g_acc[rows, pl.ds(128, 1)]
            grad = inv * scaled_image[rows] - x_acc[rows] * pull
            slots = first + lax.broadcasted_iota(jnp.int32, (ROW_STEP, block_cols), 0)
            g_own[rows] = jnp.where(slots < held, grad, 0.0).astype(bf16)

    grads = LineGather(depth, me, member, g_own, g_all, c_send, c_recv, c_turn)
    grads.start()

    def vision_term(left, right):
        return lax.dot_general(left, right, (((0,), (0,)), ((), ())), preferred_element_type=f32)

    def use_grads(block):
        vision_from_mate(block).wait_recv()
        g_acc[...] += vision_term(v_all[block], g_all[block])

    g_acc[...] = vision_term(vision_ref[:, own_cols], g_own[...])
    for step in range(1, shards):
        vision_from(step).wait_recv()
        vision_to_mate(lax.rem(me + step, shards)).start()
    for hop in range(1, depth):
        for chunk in range(CHUNKS):
            grads.relay(hop, chunk)
        if hop < depth - 1:
            grads.line_blocks(hop, use_grads)
    grads.line_blocks(depth - 1, use_grads)

    for k in range(len(order)):
        for yy in far:
            text_from_far(k, yy).wait_recv()
    t_copy.wait()

    @pl.loop(0, text_rows // ROW_STEP)
    def _(n):
        rows = pl.ds(pl.multiple_of(n * ROW_STEP, ROW_STEP), ROW_STEP)
        squares = jnp.zeros((ROW_STEP, 1), f32)
        inner = jnp.zeros((ROW_STEP, 1), f32)
        for j in range(groups):
            cols = pl.ds(j * block_cols, block_cols)
            x = tv[rows, cols].astype(f32)
            norm = own_text[j, core, y, rows].astype(f32) + mate_text[j, y, rows].astype(f32)
            for yy in far:
                norm = norm + far_text[yy, j, rows].astype(f32)
            scaled = gain_ref[:, cols] * norm
            squares += jnp.sum(x * x, axis=1, keepdims=True)
            inner += jnp.sum(x * scaled, axis=1, keepdims=True)
        inv = lax.rsqrt(squares / width + norm_eps)
        pull = inv**3 * (inner / width)
        for j in range(groups):
            cols = pl.ds(j * block_cols, block_cols)
            x = tv[rows, cols].astype(f32)
            norm = own_text[j, core, y, rows].astype(f32) + mate_text[j, y, rows].astype(f32)
            for yy in far:
                norm = norm + far_text[yy, j, rows].astype(f32)
            text_out[rows, cols] = (inv * (gain_ref[:, cols] * norm) - x * pull).astype(bf16)

    for hop in range(depth):
        grads.side_blocks(hop, use_grads)
    for c in range(fold):
        proj_out[pl.ds(c, shard_k, stride=fold), :] = g_acc[:, c * 128 : (c + 1) * 128] * grad_scale

    weights.drain()
    grads.drain()
    for step in range(1, shards):
        vision_to(step).wait_send()
        vision_to_mate(lax.rem(me + step, shards)).wait_send()
    for step in range(1, groups):
        stat_to(step).wait_send()
    for k in range(len(order)):
        text_to_mate(k).wait_send()
        for yy in far:
            text_to_far(k, yy).wait_send()
    for yy in far + [y]:
        image_to_mate(yy).wait_send()
    for yy in far:
        image_to_far(yy).wait_send()


def place_outputs(text_in, proj_in, text_out, proj_out, text_held, proj_held, in_sem, out_sem):
    def copies(refs, sem):
        found = []
        for k, (src, dst) in enumerate(refs):
            step = src.shape[0] // PIECES
            for p in range(PIECES):
                rows = pl.ds(p * step, step)
                found.append(pltpu.make_async_copy(src.at[rows], dst.at[rows], sem.at[k, p]))
        return found

    into = copies(((text_in, text_held), (proj_in, proj_held)), in_sem)
    back = copies(((text_held, text_out), (proj_held, proj_out)), out_sem)
    for copy in into:
        copy.start()
    for first, second in zip(into, back):
        first.wait()
        second.start()
    for copy in back:
        copy.wait()


def live_rows(image_count, groups):
    image_rows = IMG_MAX * PATCH
    row_ids = jnp.arange(groups * image_rows, dtype=jnp.int32)
    owners = row_ids // image_rows
    slot_ids = row_ids % image_rows // PATCH
    owner_match = owners[:, None] == jnp.arange(groups, dtype=jnp.int32)[None, :]
    owner_counts = jnp.sum(jnp.where(owner_match, image_count[None, :], 0), axis=1)
    return (slot_ids < owner_counts)[:, None]


def fused_body(vision_rows, image_count, proj_flat, text_embeds, norm_gain, q_weight, q_grad):
    groups, shards = lax.axis_size("mp"), lax.axis_size("dp")
    model_width, bc = q_weight.shape
    image_rows, enc_width = vision_rows.shape
    text_rows = text_embeds.shape[0]
    shard_k = proj_flat.shape[0] * proj_flat.shape[1] // bc
    chips, depth = groups // CORES, shards // SIDE
    grad_scale = 1.0 / float(shards * image_rows) ** 0.5
    f32, bf16 = jnp.float32, jnp.bfloat16
    vmem, dma = pltpu.VMEM, pltpu.SemaphoreType.DMA
    on_chip = pl.BlockSpec(memory_space=pltpu.VMEM)
    scalars = pl.BlockSpec(memory_space=pltpu.SMEM)
    anywhere = pl.BlockSpec(memory_space=pl.ANY)
    text_grad, proj_block = pl.pallas_call(
        functools.partial(kernel, shards, groups, grad_scale),
        name="projector_backward",
        out_shape=(
            jax.ShapeDtypeStruct(text_embeds.shape, bf16),
            jax.ShapeDtypeStruct(proj_flat.shape, f32),
        ),
        in_specs=[on_chip, on_chip, scalars, on_chip] + [anywhere] * 3,
        out_specs=(on_chip, on_chip),
        scratch_shapes=[
            vmem(q_grad.shape, bf16),
            vmem((groups, bc, bc), bf16),
            vmem(text_embeds.shape, bf16),
            vmem((groups, CORES, chips, text_rows, bc), bf16),
            vmem((groups, image_rows, bc), bf16),
            vmem((groups, chips, text_rows, bc), bf16),
            vmem((chips, image_rows, bc), bf16),
            vmem((groups, chips, text_rows, bc), bf16),
            vmem((chips, image_rows, bc), bf16),
            vmem((chips, groups, text_rows, bc), bf16),
            vmem((chips, image_rows, bc), bf16),
            vmem((image_rows, bc), f32),
            vmem((image_rows, bc), f32),
            vmem((shard_k, bc), f32),
            vmem((image_rows, bc), bf16),
            vmem((8, image_rows), f32),
            vmem((groups, 8, image_rows), f32),
            vmem((shards,) + proj_flat.shape, bf16),
            vmem(proj_flat.shape, f32),
            vmem((shards, image_rows, bc), bf16),
            vmem((shards, image_rows, shard_k), bf16),
            dma, dma((groups,)), dma,
            dma((3, depth, CHUNKS)), dma((shards, CHUNKS)), dma((2, CHUNKS)),
            dma((3, depth, CHUNKS)), dma((shards, CHUNKS)), dma((2, CHUNKS)),
            dma((shards,)), dma((shards,)), dma((shards,)), dma((shards,)),
            dma((groups,)), dma((groups,)),
            dma((chips,)), dma((chips,)),
            dma((groups, chips)), dma((chips, groups)),
            dma((chips,)), dma((chips,)),
            dma((groups,)), dma((groups,)),
        ],
        compiler_params=pltpu.CompilerParams(
            collective_id=0, has_side_effects=True, vmem_limit_bytes=56 * 1024 * 1024
        ),
    )(
        proj_flat,
        vision_rows,
        image_count,
        norm_gain[None, :],
        q_grad,
        q_weight.reshape(groups, bc, bc),
        text_embeds,
    )
    kinds = (text_grad, proj_block)
    return pl.pallas_call(
        place_outputs,
        name="place_outputs",
        out_shape=tuple(jax.ShapeDtypeStruct(a.shape, a.dtype) for a in kinds),
        in_specs=[anywhere] * 2,
        out_specs=(anywhere, anywhere),
        scratch_shapes=[vmem(a.shape, a.dtype) for a in kinds] + [dma((2, PIECES)), dma((2, PIECES))],
    )(*kinds)


def norm_back(rows_in, grads, gain):
    inputs = rows_in.astype(jnp.float32)
    inv_rms = lax.rsqrt(jnp.mean(inputs * inputs, axis=-1, keepdims=True) + norm_eps)
    scaled = gain[None, :] * grads
    inner_mean = jnp.mean(scaled * inputs, axis=-1, keepdims=True)
    return inv_rms * scaled - inputs * inv_rms**3 * inner_mean


def general_body(vision_rows, image_count, proj_flat, text_embeds, norm_gain, q_weight, q_grad):
    groups = lax.axis_size("mp")
    member = lax.axis_index("mp")
    shards = lax.axis_size("dp")
    enc_width = vision_rows.shape[1]
    block_cols = q_weight.shape[1]
    model_width = q_weight.shape[0]
    used_count = enc_width * block_cols
    image_rows = IMG_MAX * PATCH
    gathered = lax.all_gather(proj_flat, "dp", axis=0, tiled=True)
    proj_block = gathered.reshape(-1)[:used_count].reshape(enc_width, block_cols)
    embed_cols = jnp.dot(vision_rows, proj_block, preferred_element_type=jnp.float32).astype(
        jnp.bfloat16
    )
    live_group = live_rows(image_count, groups)
    blocks = q_grad.reshape(groups, ROWS_DEV, block_cols)
    image_query = blocks[:, :image_rows].reshape(-1, block_cols)
    text_query = blocks[:, image_rows:].reshape(-1, block_cols)
    image_term = row_term(image_query, q_weight)
    image_norm = lax.psum_scatter(
        image_term.astype(jnp.bfloat16), "mp", scatter_dimension=1, tiled=True
    ).astype(jnp.float32)
    text_norm = lax.psum_scatter(
        row_term(text_query, q_weight).astype(jnp.bfloat16), "mp", scatter_dimension=0, tiled=True
    ).astype(jnp.float32)
    x_cols = embed_cols.astype(jnp.float32)
    gain_cols = lax.dynamic_slice_in_dim(norm_gain, member * block_cols, block_cols)
    scaled = gain_cols[None, :] * image_norm
    squares, inner_sum = lax.psum(
        (jnp.sum(x_cols * x_cols, axis=1), jnp.sum(scaled * x_cols, axis=1)), "mp"
    )
    inv_rms = lax.rsqrt(squares / model_width + norm_eps)[:, None]
    image_input = inv_rms * scaled - x_cols * inv_rms**3 * (inner_sum / model_width)[:, None]
    image_cols = jnp.where(live_group, image_input, 0.0).astype(jnp.bfloat16)
    text_grad = norm_back(text_embeds, text_norm, norm_gain).astype(jnp.bfloat16)
    grad_scale = 1.0 / jnp.sqrt(jnp.float32(shards * groups * image_rows))
    proj_part = (
        lax.dot_general(
            vision_rows, image_cols, (((0,), (0,)), ((), ())), preferred_element_type=jnp.float32
        )
        * grad_scale
    )
    stored_rows = proj_flat.shape[0]
    padded = jnp.pad(proj_part.reshape(-1), (0, shards * stored_rows * 128 - used_count))
    padded = padded.reshape(shards * stored_rows, 128)
    proj_grad = lax.psum_scatter(padded, "dp", scatter_dimension=0, tiled=True)
    return (text_grad, proj_grad)


def body(vision_rows, image_count, proj_flat, text_embeds, norm_gain, q_weight, q_grad):
    groups, shards = lax.axis_size("mp"), lax.axis_size("dp")
    bc = q_weight.shape[1]
    count = proj_flat.shape[0] * proj_flat.shape[1]
    shard_k = count // bc
    fits = (
        count % bc == 0
        and shard_k % 128 == 0
        and shard_k * shards == vision_rows.shape[1]
        and shard_k == vision_rows.shape[0]
        and bc % TILE == 0
        and groups > CORES
        and groups % CORES == 0
        and vision_rows.shape[0] // groups % ROW_STEP == 0
        and text_embeds.shape[0] % (PIECES * ROW_STEP) == 0
        and shards > SIDE
        and shards % SIDE == 0
    )
    run = fused_body if fits else general_body
    return run(vision_rows, image_count, proj_flat, text_embeds, norm_gain, q_weight, q_grad)


def solution(mesh):
    return jax.shard_map(
        body,
        mesh=mesh,
        in_specs=(
            P("dp", None),
            P("dp"),
            P(("dp", "mp"), None),
            P(("dp", "mp"), None),
            P(),
            P(None, "mp"),
            P("dp", "mp"),
        ),
        out_specs=(P(("dp", "mp"), None), P(("dp", "mp"), None)),
        check_vma=False,
    )
```
